16 devices in a mesh: rep: 1, r: 4 (over y, z), s: 4 (over x, core).
Axes of the slice: x: 2, y: 2, z: 2, core: 2. Of those that a mesh axis runs over, the one named last changes fastest.
Arguments:
- x: bfloat16 [16, 4096, 640], P(('rep', 'r', 's'))
- dy: bfloat16 [16, 4096, 640], P(('rep', 'r', 's'))
- w_gate: bfloat16 [2, 640, 3200], P(None, 's')
- w_up: bfloat16 [2, 640, 3200], P(None, 's')
- w_down: bfloat16 [2, 3200, 640], P(None, 's')
- m_w_gate: float32 [2, 640, 3200], P(None, 's')
- m_w_up: float32 [2, 640, 3200], P(None, 's')
- m_w_down: float32 [2, 3200, 640], P(None, 's')
- v_w_gate: float32 [2, 640, 3200], P(None, 's')
- v_w_up: float32 [2, 640, 3200], P(None, 's')
- v_w_down: float32 [2, 3200, 640], P(None, 's')
Outputs:
- output 1: bfloat16 [2, 640, 3200], P('rep', 's')
- output 2: bfloat16 [2, 640, 3200], P('rep', 's')
- output 3: bfloat16 [2, 3200, 640], P('rep', 's')
- output 4: float32 [2, 640, 3200], P('rep', 's')
- output 5: float32 [2, 640, 3200], P('rep', 's')
- output 6: float32 [2, 3200, 640], P('rep', 's')
- output 7: float32 [2, 640, 3200], P('rep', 's')
- output 8: float32 [2, 640, 3200], P('rep', 's')
- output 9: float32 [2, 3200, 640], P('rep', 's')
All inputs are finite; a program needn't handle non-finite values.
Results may differ from the reference program's by a relative error of at most 0.0223.
Values are sent between devices in bfloat16 or wider.
A program may use at most 2 GiB of HBM per device.

```python
import jax
import jax.numpy as jnp
from jax import lax

SEQUENCES = 16
TOKENS = 4096
D = 640
FF = 3200
LAYERS = 2
NAMES = ("w_gate", "w_up", "w_down")
SHAPES = {"w_gate": (LAYERS, D, FF), "w_up": (LAYERS, D, FF), "w_down": (LAYERS, FF, D)}


def bump(key, n, height):
    away = (jnp.arange(n, dtype=jnp.int32) - jax.random.randint(key, (), 0, n, jnp.int32)) % n
    return jnp.where(away < n // 8, height, 1.0)


def together(key, own, strength):
    shared = jax.random.normal(key, own.shape[1:], jnp.float32)
    return (own + strength * shared) * lax.rsqrt(1 + strength * strength)


def setup_inputs(seed: int = 0, part: int = 0) -> dict:
    kx, kdy, ka, kb, kz, kf, kh, kl, *keys = jax.random.split(jax.random.key(seed), 8 + 3 * len(NAMES))
    kx, kdy, ka, kb = (jax.random.fold_in(k, part) for k in (kx, kdy, ka, kb))
    kw, km, kv = (keys[i::3] for i in range(3))
    shape = (SEQUENCES, TOKENS, D)
    much_x, much_dy = jax.random.uniform(kz, (2,), jnp.float32, 0.0, 1.0)
    loud = 2.0 ** jax.random.uniform(jax.random.fold_in(kz, 1), (), jnp.float32, -1.0, 2.0)
    layers = 2.0 ** jax.random.uniform(kl, (LAYERS, 1, 1), jnp.float32, -1.0, 1.0)
    x = together(ka, jax.random.normal(kx, shape, jnp.float32), much_x) * bump(kf, D, 4.0)
    dy = together(kb, jax.random.normal(kdy, shape, jnp.float32), much_dy)
    drawn = {"x": x.astype(jnp.bfloat16), "dy": (loud * dy * (SEQUENCES * TOKENS) ** -0.5).astype(jnp.bfloat16)}
    for key, name in zip(kw, NAMES, strict=True):
        w = jax.random.normal(key, SHAPES[name], jnp.float32) * SHAPES[name][1] ** -0.5
        drawn[name] = (w * {"w_gate": 1.0, "w_up": bump(kh, FF, 4.0), "w_down": layers}[name]).astype(jnp.bfloat16)
    for key, name in zip(km, NAMES, strict=True):
        drawn[f"m_{name}"] = 0.1 * jax.random.normal(key, SHAPES[name], jnp.float32)
    for key, name in zip(kv, NAMES, strict=True):
        drawn[f"v_{name}"] = jax.random.uniform(key, SHAPES[name], jnp.float32, 0.005, 0.015)
    return drawn


def matmul(a, w):
    return jnp.dot(a, w, preferred_element_type=jnp.float32).astype(jnp.bfloat16)


def normed(h):
    wide = h.astype(jnp.float32)
    scale = lax.rsqrt(jnp.mean(wide**2, -1, keepdims=True) + 1e-6)
    return (wide * scale).astype(jnp.bfloat16)


def layer(h, w):
    a = normed(h)
    gate = jnp.dot(a, w["w_gate"], preferred_element_type=jnp.float32)
    up = jnp.dot(a, w["w_up"], preferred_element_type=jnp.float32)
    return h + matmul((jax.nn.silu(gate) * up).astype(jnp.bfloat16), w["w_down"])


def adamw(w, m, v, g):
    m = 0.9 * m + 0.1 * g
    v = 0.95 * v + 0.05 * g * g
    step = m * lax.rsqrt(v + 1e-8) + 0.1 * w
    return (w - 0.02 * step).astype(jnp.bfloat16), m, v


def stack(weights, h):
    return lax.scan(lambda h, w: (layer(h, w), None), h, weights)[0]


def reference(x, dy, w_gate, w_up, w_down, m_w_gate, m_w_up, m_w_down, v_w_gate, v_w_up, v_w_down):
    weights = dict(zip(NAMES, (w_gate, w_up, w_down), strict=True))

    def take(so_far, sequence):
        h, by_y = sequence
        _, back = jax.vjp(lambda w: stack(w, h), weights)
        return jax.tree.map(lambda total, term: total + term.astype(jnp.float32), so_far, back(by_y)[0]), None

    none_yet = {name: jnp.zeros(w.shape, jnp.float32) for name, w in weights.items()}
    by_weights, _ = lax.scan(take, none_yet, (x, dy))
    gradients = [by_weights[name].astype(jnp.bfloat16).astype(jnp.float32) for name in NAMES]
    new = [
        adamw(w.astype(jnp.float32), m, v, g)
        for w, m, v, g in zip((w_gate, w_up, w_down), (m_w_gate, m_w_up, m_w_down), (v_w_gate, v_w_up, v_w_down), gradients, strict=True)
    ]
    return tuple(one[which] for which in range(3) for one in new)
```

```python
import functools

import jax
import jax.numpy as jnp
from jax import lax
from jax.experimental import pallas as pl
from jax.experimental.pallas import tpu as pltpu
from jax.sharding import PartitionSpec as P

MESH = pl.DeviceIdType.MESH
F32, BF16 = jnp.float32, jnp.bfloat16
VMEM_LIMIT = 67043328


def dot(a, b, over_a, over_b):
    return lax.dot_general(a, b, (((over_a,), (over_b,)), ((), ())), preferred_element_type=F32)


def sigmoid(g):
    return 0.5 * jnp.tanh(0.5 * g) + 0.5


def scale_of(wide):
    return lax.rsqrt(jnp.mean(wide * wide, -1, keepdims=True) + 1e-6)


def places():
    s, r = lax.axis_index("s"), lax.axis_index("r")
    other = s + 1 - 2 * lax.rem(s, 2)
    return s, r, other, lax.rem(s + 2, 4), lax.rem(r + 2, 4), r + 1 - 2 * lax.rem(r, 2)


def remote(src, dst, send, recv, **where):
    return pltpu.make_async_remote_copy(src_ref=src, dst_ref=dst, send_sem=send, recv_sem=recv, device_id=where, device_id_type=MESH)


def greet(*peers):
    barrier = pltpu.get_barrier_semaphore()
    for peer in peers:
        pl.semaphore_signal(barrier, inc=1, device_id=peer, device_id_type=MESH)
    pl.semaphore_wait(barrier, len(peers))


def forward_kernel(sizes, x_ref, wg_ref, wu_ref, wd_ref, h_ref, w_gu, w_d, a_s, hid_s, gu_s, d_s, own_sem, out_sem, x_send, x_recv, y_send, y_recv, c_send, c_recv):
    tokens, d, ff, chunk, chunks, block = sizes
    steps = tokens // block
    c, t = pl.program_id(0), pl.program_id(1)
    s, r, other, across, by_y, _ = places()
    y = lax.div(r, 2)
    rows_gu, rows_d = d // 4, ff // 4
    pieces = 2 * chunks + 2
    first_1 = chunks + 2

    def parts(p, holder, half):
        n_gu, n_d = rows_gu // 2, rows_d // 2
        at_gu = pl.ds(pl.multiple_of(holder * rows_gu + half * n_gu, 16), n_gu)
        at_d = pl.ds(pl.multiple_of(holder * rows_d + half * n_d, 16), n_d)
        if p < chunks:
            return [gu_s.at[p, at_gu]]
        if p == chunks:
            return [d_s.at[at_d]]
        if p == chunks + 1:
            return [w_d.at[0, at_d]]
        return [w_gu.at[p - first_1, at_gu]]

    def own(p, half):
        n_gu, n_d = rows_gu // 2, rows_d // 2
        at_gu = pl.ds(pl.multiple_of(half * n_gu, 16), n_gu)
        at_d = pl.ds(pl.multiple_of(half * n_d, 16), n_d)
        to = parts(p, s, half)[0]
        if p in (chunks, chunks + 1):
            return [(wd_ref.at[p - chunks, at_d], to)]
        layer, n = (0, p) if p < chunks else (1, p - first_1)
        cols = pl.ds(n * chunk, chunk)
        return [(wg_ref.at[layer, at_gu, cols], to.at[:, pl.ds(0, chunk)]), (wu_ref.at[layer, at_gu, cols], to.at[:, pl.ds(chunk, chunk)])]

    def own_whole(p):
        at_gu = pl.ds(pl.multiple_of(s * rows_gu, 16), rows_gu)
        at_d = pl.ds(pl.multiple_of(s * rows_d, 16), rows_d)
        if p in (chunks, chunks + 1):
            return [(wd_ref.at[p - chunks], (d_s if p == chunks else w_d.at[0]).at[at_d])]
        layer, n = (0, p) if p < chunks else (1, p - first_1)
        to = (gu_s.at[p] if p < chunks else w_gu.at[p - first_1]).at[at_gu]
        cols = pl.ds(n * chunk, chunk)
        return [(wg_ref.at[layer, :, cols], to.at[:, pl.ds(0, chunk)]), (wu_ref.at[layer, :, cols], to.at[:, pl.ds(chunk, chunk)])]

    def own_copies(p):
        return [pltpu.make_async_copy(a, b, own_sem.at[p, i]) for i, (a, b) in enumerate(own_whole(p))]

    def x_copies(p):
        return [remote(a, b, x_send.at[p, i], x_recv.at[p, i], s=across) for i, (a, b) in enumerate(own(p, y))]

    def own_to_core(p):
        return [remote(a, b, c_send.at[p, i], c_recv.at[p, i], s=other) for i, (a, b) in enumerate(own_whole(p))]

    def y_copy(p):
        ref = parts(p, across, y)[0]
        return remote(ref, ref, y_send.at[p], y_recv.at[p], r=by_y)

    def to_core(p, half, i):
        ref = parts(p, across, half)[0]
        return remote(ref, ref, c_send.at[p, 2 + i], c_recv.at[p, 2 + i], s=other)

    def out_copy(p):
        if p < chunks:
            return pltpu.make_async_copy(gu_s.at[p], w_gu.at[chunks + p], out_sem.at[p])
        return pltpu.make_async_copy(d_s, w_d.at[1], out_sem.at[p])

    def x_done(p):
        for copy in x_copies(p):
            copy.wait()
        y_copy(p).start()
        to_core(p, y, 0).start()

    def y_done(p):
        y_copy(p).wait()
        to_core(p, 1 - y, 1).start()

    def ready(p):
        for copy in own_copies(p) + own_to_core(p) + [to_core(p, y, 0), to_core(p, 1 - y, 1)]:
            copy.wait()
        if p <= chunks:
            out_copy(p).start()

    def at(cc, tt, do, *pieces_of):
        @pl.when((c == cc) & (t == tt))
        def _():
            for p in pieces_of:
                do(p)

    @pl.when((c == 0) & (t == 0))
    def _():
        greet({"s": other}, {"s": across}, {"r": by_y})
        for p in range(pieces):
            for copy in x_copies(p) + own_to_core(p) + own_copies(p):
                copy.start()

    @pl.when(c == 0)
    def _():
        wide = x_ref[...].astype(F32)
        a_s[pl.ds(pl.multiple_of(t * block, block), block)] = (wide * scale_of(wide)).astype(BF16)

    at(0, 0, x_done, 0)
    at(0, 0, y_done, 0)
    for n in range(chunks):
        at(n, 0, ready, n)
        if n + 1 < chunks:
            at(n, 1, x_done, n + 1)
            at(n, 3, y_done, n + 1)
    at(chunks - 1, 0, x_done, chunks)
    at(chunks - 1, 3, y_done, chunks)
    at(chunks - 1, 3, x_done, chunks + 1)
    at(chunks, 0, ready, chunks)
    at(chunks, 0, y_done, chunks + 1)
    at(chunks, 0, x_done, chunks + 2)
    at(chunks, 1, y_done, chunks + 2)
    at(chunks, 1, x_done, chunks + 3)
    at(chunks, 2, y_done, chunks + 3)
    at(chunks, 2, x_done, chunks + 4, chunks + 5)
    at(chunks, 3, y_done, chunks + 4, chunks + 5)
    at(chunks, 3, x_done, chunks + 6)

    rows = pl.ds(pl.multiple_of(t * block, block), block)

    @pl.when(c < chunks)
    def _():
        gu = dot(a_s[rows], gu_s[c], 1, 0)
        g, u = gu[:, :chunk], gu[:, chunk:]
        hid_s[rows, pl.ds(pl.multiple_of(c * chunk, 128), chunk)] = (g * sigmoid(g) * u).astype(BF16)

    @pl.when(c == chunks)
    def _():
        added = dot(hid_s[rows], d_s[...], 1, 0).astype(BF16)
        h_ref[...] = (x_ref[...].astype(F32) + added.astype(F32)).astype(BF16)

    at(chunks, steps - 1, y_done, chunks + 6)
    at(chunks, steps - 1, ready, *range(chunks + 1, pieces))

    @pl.when((c == chunks) & (t == steps - 1))
    def _():
        for p in range(chunks + 1):
            out_copy(p).wait()


def forward(x, wg, wu, wd, chunk, block):
    (tokens, d), ff = x.shape, wg.shape[-1]
    chunks = ff // chunk
    pieces = 2 * chunks + 2
    sizes = (tokens, d, ff, chunk, chunks, block)
    whole = lambda a: pl.BlockSpec(a.shape, lambda c, t: (0,) * a.ndim, pipeline_mode=pl.Buffered(1))
    dma = pltpu.SemaphoreType.DMA
    return pl.pallas_call(
        functools.partial(forward_kernel, sizes),
        grid=(chunks + 1, tokens // block),
        in_specs=[pl.BlockSpec((block, d), lambda c, t: (jnp.where((c == 0) | (c == chunks), t, 0), 0)), whole(wg), whole(wu), whole(wd)],
        out_specs=[
            pl.BlockSpec((block, d), lambda c, t: (jnp.where(c == chunks, t, 0), 0)),
            pl.BlockSpec(memory_space=pl.ANY),
            pl.BlockSpec(memory_space=pl.ANY),
        ],
        out_shape=[
            jax.ShapeDtypeStruct((tokens, d), BF16),
            jax.ShapeDtypeStruct((2 * chunks, d, 2 * chunk), BF16),
            jax.ShapeDtypeStruct((2, ff, d), BF16),
        ],
        scratch_shapes=[
            pltpu.VMEM((tokens, d), BF16),
            pltpu.VMEM((tokens, ff), BF16),
            pltpu.VMEM((chunks, d, 2 * chunk), BF16),
            pltpu.VMEM((ff, d), BF16),
            dma((pieces, 2)),
            dma((chunks + 1,)),
            dma((pieces, 2)),
            dma((pieces, 2)),
            dma((pieces,)),
            dma((pieces,)),
            dma((pieces, 4)),
            dma((pieces, 4)),
        ],
        compiler_params=pltpu.CompilerParams(collective_id=0, has_side_effects=True, vmem_limit_bytes=VMEM_LIMIT),
        name="forward",
    )(x, wg, wu, wd)


def backward_kernel(sizes, h_ref, dy_ref, x_ref, wgu_ref, wd_ref, gg, gu, gd, a_s, dy_s, da_s, acc_s, mine, c_out, c_in, x_out, x_in, y_out, y_in, z_out, z_in, done,
                    c_sem, x_sem, y_sem, z_sem, d_send, d_recv, l_sem):
    tokens, d, ff, chunk, chunks, block, sub = sizes
    last, steps = 2 * chunks - 1, tokens // block
    c, t = pl.program_id(0), pl.program_id(1)
    s, r, other, across, by_y, by_z = places()
    x, core = lax.div(s, 2), lax.rem(s, 2)
    n = d // 4
    rows = pl.ds(pl.multiple_of(t * block, block), block)

    def to_core(k):
        return remote(c_out, c_in.at[lax.rem(k, 2)], c_sem.at[0], c_sem.at[1 + lax.rem(k, 2)], s=other)

    def to_x(k):
        return remote(x_out, x_in.at[lax.rem(k, 2)], x_sem.at[0], x_sem.at[1 + lax.rem(k, 2)], s=across)

    def to_y(k):
        return remote(y_out, y_in.at[lax.rem(k, 2)], y_sem.at[0], y_sem.at[1 + lax.rem(k, 2)], r=by_y)

    def to_z(k):
        return remote(z_out, z_in.at[lax.rem(k, 2)], z_sem.at[0], z_sem.at[1 + lax.rem(k, 2)], r=by_z)

    def finals(k):
        layer, of = 1 - lax.div(k, chunks), lax.rem(k, chunks)
        cols = pl.ds(pl.multiple_of(of * chunk, 128), chunk)
        number = 4 * of + s
        owner, place = lax.div(number, chunks), lax.rem(number, chunks)
        to = gd.at[layer, pl.ds(pl.multiple_of(place * n, 16), n)]
        down = done.at[:, pl.ds(2 * chunk, d)]
        here = [
            pltpu.make_async_copy(done.at[:, pl.ds(0, chunk)], gg.at[layer, :, cols], l_sem.at[0]),
            pltpu.make_async_copy(done.at[:, pl.ds(chunk, chunk)], gu.at[layer, :, cols], l_sem.at[1]),
        ]
        return here, owner == s, pltpu.make_async_copy(down, to, l_sem.at[2]), remote(down, to, d_send, d_recv.at[layer, place], s=owner)

    def start_finals(k):
        here, stays, local, away = finals(k)
        for copy in here:
            copy.start()
        pl.when(stays)(local.start)
        pl.when(jnp.logical_not(stays))(away.start)

    def end_finals(k):
        here, stays, local, away = finals(k)
        for copy in here:
            copy.wait()
        pl.when(stays)(local.wait)
        pl.when(jnp.logical_not(stays))(away.wait_send)

    @pl.when((c == 0) & (t == 0))
    def _():
        greet({"s": other}, {"s": across}, {"s": 3 - s}, {"r": by_y}, {"r": by_z})

    @pl.when((t == 1) & (c >= 2))
    def _():
        k = c - 2
        to_y(k).wait()
        z_out[...] = (y_out[...].astype(F32) + y_in[lax.rem(k, 2)].astype(F32)).astype(BF16)
        to_z(k).start()

    @pl.when((t == 1) & (c >= 1) & (c <= last + 1))
    def _():
        k = c - 1
        to_core(k).wait()
        x_out[...] = (mine[1 - x] + c_in[lax.rem(k, 2), 1 - x].astype(F32)).astype(BF16)
        to_x(k).start()
        mine[x] += c_in[lax.rem(k, 2), x].astype(F32)

    @pl.when((t == 3) & (c >= 2))
    def _():
        k = c - 2
        to_z(k).wait()
        pl.when(k >= 1)(lambda: end_finals(k - 1))
        done[...] = (z_out[...].astype(F32) + z_in[lax.rem(k, 2)].astype(F32)).astype(BF16)
        start_finals(k)

    @pl.when((t == 3) & (c >= 1) & (c <= last + 1))
    def _():
        k = c - 1
        to_x(k).wait()
        y_out[...] = (mine[x] + x_in[lax.rem(k, 2)].astype(F32)).astype(BF16)
        to_y(k).start()

    @pl.when(c == 0)
    def _():
        wide = h_ref[...].astype(F32)
        a_s[rows] = (wide * scale_of(wide)).astype(BF16)
        dy_s[rows] = dy_ref[...]
        da_s[rows] = jnp.zeros((block, d), F32)

    @pl.when(c == chunks)
    def _():
        wide = x_ref[...].astype(F32)
        a_s[rows] = (wide * scale_of(wide)).astype(BF16)

    @pl.when(c <= last)
    def _():
        @pl.when(t == 0)
        def _():
            acc_s[...] = jnp.zeros_like(acc_s)

        for i in range(block // sub):
            at = pl.ds(pl.multiple_of(t * block + i * sub, sub), sub)
            a, dy = a_s[at], dy_s[at]
            both = dot(a, wgu_ref[0], 1, 0)
            dh = dot(dy, wd_ref[0], 1, 1).astype(BF16).astype(F32)
            g, u = both[:, :chunk], both[:, chunk:]
            sg = sigmoid(g)
            sl = g * sg
            hid = (sl * u).astype(BF16)
            by_u = (dh * sl).astype(BF16)
            by_g = (dh * u * (sg * (1 + g * (1 - sg)))).astype(BF16)
            by_gu = jnp.concatenate([by_g, by_u], 1)
            acc_s[:, : 2 * chunk] += dot(a, by_gu, 0, 0)
            acc_s[:, 2 * chunk :] += dot(hid, dy, 0, 0)

            @pl.when(c < chunks)
            def _():
                da_s[at] += dot(by_gu, wgu_ref[0], 1, 1)

        @pl.when(c == chunks - 1)
        def _():
            da = da_s[rows].astype(BF16).astype(F32)
            wide = h_ref[...].astype(F32)
            scale = scale_of(wide)
            along = jnp.sum(da * wide, -1, keepdims=True) * (scale * scale * scale) * (1.0 / d)
            dy_s[rows] = (dy_s[rows].astype(F32) + (da * scale - wide * along).astype(BF16).astype(F32)).astype(BF16)

        @pl.when(t == steps - 1)
        def _():
            for i in range(2):
                mine[i] = acc_s[pl.ds(pl.multiple_of((2 * i + core) * n, 8), n)]
                c_out[i] = acc_s[pl.ds(pl.multiple_of((2 * i + 1 - core) * n, 8), n)].astype(BF16)
            to_core(c).start()

    @pl.when((c == last + 2) & (t == steps - 1))
    def _():
        end_finals(last)
        for layer in range(2):
            for place in range(chunks):
                number = s * chunks + place
                to = gd.at[layer, pl.ds(place * n, n)]
                from_other = lax.rem(number, 4) != s
                copy = remote(done.at[:, pl.ds(2 * chunk, d)], to, d_send, d_recv.at[layer, place], s=other)
                pl.when(from_other)(copy.wait_recv)


def backward(h, dy, x, wgu, wd, chunk, block, sub):
    (tokens, d), ff = x.shape, wd.shape[1]
    chunks = ff // chunk
    n, last = d // 4, 2 * chunks - 1
    sizes = (tokens, d, ff, chunk, chunks, block, sub)
    dma = pltpu.SemaphoreType.DMA
    wide = 2 * chunk + d
    at = lambda *when: pl.BlockSpec((block, d), lambda c, t: (jnp.where(functools.reduce(jnp.logical_or, [c == w for w in when]), t, 0), 0))
    return pl.pallas_call(
        functools.partial(backward_kernel, sizes),
        grid=(last + 3, tokens // block),
        in_specs=[
            at(0, chunks - 1),
            at(0),
            at(chunks),
            pl.BlockSpec((1, d, 2 * chunk), lambda c, t: (jnp.minimum(c, last), 0, 0)),
            pl.BlockSpec((1, chunk, d), lambda c, t: (lax.div(jnp.minimum(c, last), chunks), lax.rem(jnp.minimum(c, last), chunks), 0)),
        ],
        out_specs=[pl.BlockSpec(memory_space=pl.ANY)] * 3,
        out_shape=[
            jax.ShapeDtypeStruct((2, n, ff), BF16),
            jax.ShapeDtypeStruct((2, n, ff), BF16),
            jax.ShapeDtypeStruct((2, ff // 4, d), BF16),
        ],
        scratch_shapes=[
            pltpu.VMEM((tokens, d), BF16),
            pltpu.VMEM((tokens, d), BF16),
            pltpu.VMEM((tokens, d), F32),
            pltpu.VMEM((d, wide), F32),
            pltpu.VMEM((2, n, wide), F32),
            pltpu.VMEM((2, n, wide), BF16),
            pltpu.VMEM((2, 2, n, wide), BF16),
            pltpu.VMEM((n, wide), BF16),
            pltpu.VMEM((2, n, wide), BF16),
            pltpu.VMEM((n, wide), BF16),
            pltpu.VMEM((2, n, wide), BF16),
            pltpu.VMEM((n, wide), BF16),
            pltpu.VMEM((2, n, wide), BF16),
            pltpu.VMEM((n, wide), BF16),
            dma((3,)),
            dma((3,)),
            dma((3,)),
            dma((3,)),
            dma,
            dma((2, chunks)),
            dma((3,)),
        ],
        compiler_params=pltpu.CompilerParams(collective_id=1, has_side_effects=True, vmem_limit_bytes=VMEM_LIMIT),
        name="backward",
    )(h, dy, x, wgu, wd)


def adamw(w, m, v, g):
    m = 0.9 * m + 0.1 * g
    v = 0.95 * v + 0.05 * g * g
    step = m * lax.rsqrt(v + 1e-8) + 0.1 * w
    return (w - 0.02 * step).astype(BF16), m, v


def solution(mesh):
    def step(x, dy, *arrays):
        weights, m, v = (arrays[i : i + 3] for i in (0, 3, 6))
        x, dy = x[0], dy[0]
        h, wgu, wd = forward(x, *weights, 640, 1024)
        gradients = backward(h, dy, x, wgu, wd, 640, 1024, 512)
        new = [adamw(w.astype(F32), m, v, g.astype(F32)) for w, m, v, g in zip(weights, m, v, gradients, strict=True)]
        return tuple(one[which] for which in range(3) for one in new)

    states, cut = P(("rep", "r", "s"), None, None), P(None, "s", None)
    return jax.shard_map(
        step,
        mesh=mesh,
        in_specs=(states, states) + (cut,) * 9,
        out_specs=(P("rep", "s", None),) * 9,
        check_vma=False,
    )
```

```python
import functools

import jax
import jax.numpy as jnp
from jax import lax
from jax.experimental import pallas as pl
from jax.experimental.pallas import tpu as pltpu
from jax.sharding import PartitionSpec as P

MESH = pl.DeviceIdType.MESH
F32, BF16 = jnp.float32, jnp.bfloat16
VMEM_LIMIT = 67043328


def dot(a, b, over_a, over_b):
    return lax.dot_general(a, b, (((over_a,), (over_b,)), ((), ())), preferred_element_type=F32)


def sigmoid(g):
    return 0.5 * jnp.tanh(0.5 * g) + 0.5


def scale_of(wide):
    return lax.rsqrt(jnp.mean(wide * wide, -1, keepdims=True) + 1e-6)


def places():
    s, r = lax.axis_index("s"), lax.axis_index("r")
    other = s + 1 - 2 * lax.rem(s, 2)
    return s, r, other, lax.rem(s + 2, 4), lax.rem(r + 2, 4), r + 1 - 2 * lax.rem(r, 2)


def remote(src, dst, send, recv, **where):
    return pltpu.make_async_remote_copy(src_ref=src, dst_ref=dst, send_sem=send, recv_sem=recv, device_id=where, device_id_type=MESH)


def greet(*peers):
    barrier = pltpu.get_barrier_semaphore()
    for peer in peers:
        pl.semaphore_signal(barrier, inc=1, device_id=peer, device_id_type=MESH)
    pl.semaphore_wait(barrier, len(peers))


def forward_kernel(sizes, x_ref, wg_ref, wu_ref, wd_ref, h_ref, w_gu, w_d, a_s, hid_s, gu_s, d_s, own_sem, out_sem, x_send, x_recv, y_send, y_recv, c_send, c_recv):
    tokens, d, ff, chunk, chunks, block, sub = sizes
    steps = tokens // block
    c, t = pl.program_id(0), pl.program_id(1)
    s, r, other, across, by_y, _ = places()
    y = lax.div(r, 2)
    rows_gu, rows_d = d // 4, ff // 4
    pieces = 2 * chunks + 2
    first_1 = chunks + 2

    def parts(p, holder, half):
        n_gu, n_d = rows_gu // 2, rows_d // 2
        at_gu = pl.ds(pl.multiple_of(holder * rows_gu + half * n_gu, 16), n_gu)
        at_d = pl.ds(pl.multiple_of(holder * rows_d + half * n_d, 16), n_d)
        if p < chunks:
            return [gu_s.at[p, at_gu]]
        if p == chunks:
            return [d_s.at[at_d]]
        if p == chunks + 1:
            return [w_d.at[0, at_d]]
        return [w_gu.at[p - first_1, at_gu]]

    def own(p, half):
        n_gu, n_d = rows_gu // 2, rows_d // 2
        at_gu = pl.ds(pl.multiple_of(half * n_gu, 16), n_gu)
        at_d = pl.ds(pl.multiple_of(half * n_d, 16), n_d)
        to = parts(p, s, half)[0]
        if p in (chunks, chunks + 1):
            return [(wd_ref.at[p - chunks, at_d], to)]
        layer, n = (0, p) if p < chunks else (1, p - first_1)
        cols = pl.ds(n * chunk, chunk)
        return [(wg_ref.at[layer, at_gu, cols], to.at[:, pl.ds(0, chunk)]), (wu_ref.at[layer, at_gu, cols], to.at[:, pl.ds(chunk, chunk)])]

    def own_whole(p):
        at_gu = pl.ds(pl.multiple_of(s * rows_gu, 16), rows_gu)
        at_d = pl.ds(pl.multiple_of(s * rows_d, 16), rows_d)
        if p in (chunks, chunks + 1):
            return [(wd_ref.at[p - chunks], (d_s if p == chunks else w_d.at[0]).at[at_d])]
        layer, n = (0, p) if p < chunks else (1, p - first_1)
        to = (gu_s.at[p] if p < chunks else w_gu.at[p - first_1]).at[at_gu]
        cols = pl.ds(n * chunk, chunk)
        return [(wg_ref.at[layer, :, cols], to.at[:, pl.ds(0, chunk)]), (wu_ref.at[layer, :, cols], to.at[:, pl.ds(chunk, chunk)])]

    def own_copies(p):
        return [pltpu.make_async_copy(a, b, own_sem.at[p, i]) for i, (a, b) in enumerate(own_whole(p))]

    def x_copies(p):
        return [remote(a, b, x_send.at[p, i], x_recv.at[p, i], s=across) for i, (a, b) in enumerate(own(p, y))]

    def own_to_core(p):
        return [remote(a, b, c_send.at[p, i], c_recv.at[p, i], s=other) for i, (a, b) in enumerate(own_whole(p))]

    def y_copy(p):
        ref = parts(p, across, y)[0]
        return remote(ref, ref, y_send.at[p], y_recv.at[p], r=by_y)

    def to_core(p, half, i):
        ref = parts(p, across, half)[0]
        return remote(ref, ref, c_send.at[p, 2 + i], c_recv.at[p, 2 + i], s=other)

    def out_copy(p):
        if p < chunks:
            return pltpu.make_async_copy(gu_s.at[p], w_gu.at[chunks + p], out_sem.at[p])
        return pltpu.make_async_copy(d_s, w_d.at[1], out_sem.at[p])

    def x_done(p):
        for copy in x_copies(p):
            copy.wait()
        y_copy(p).start()
        to_core(p, y, 0).start()

    def y_done(p):
        y_copy(p).wait()
        to_core(p, 1 - y, 1).start()

    def ready(p):
        for copy in own_copies(p) + own_to_core(p) + [to_core(p, y, 0), to_core(p, 1 - y, 1)]:
            copy.wait()
        if p <= chunks:
            out_copy(p).start()

    def at(cc, tt, do, *pieces_of):
        @pl.when((c == cc) & (t == tt))
        def _():
            for p in pieces_of:
                do(p)

    @pl.when((c == 0) & (t == 0))
    def _():
        greet({"s": other}, {"s": across}, {"r": by_y})
        for p in range(pieces):
            for copy in x_copies(p) + own_to_core(p) + own_copies(p):
                copy.start()

    @pl.when(c == 0)
    def _():
        wide = x_ref[...].astype(F32)
        a_s[pl.ds(pl.multiple_of(t * block, block), block)] = (wide * scale_of(wide)).astype(BF16)

    last = chunks - 1
    for cc, tt, do, p in (
        (0, 0, x_done, 0), (0, 0, x_done, 1), (0, 0, y_done, 0), (0, 0, ready, 0), (0, 1, x_done, 2), (0, 2, y_done, 1), (0, 2, x_done, 3), (0, 3, x_done, 4),
        (1, 0, ready, 1), (1, 0, y_done, 2), (1, 1, y_done, 3), (1, 3, y_done, 4), (1, 3, x_done, 5), (2, 0, ready, 2),
        (3, 0, ready, 3), (3, 0, y_done, 5), (3, 0, x_done, 6), (3, 1, x_done, 7), (3, 2, x_done, 8), (4, 0, ready, 4), (4, 0, x_done, 9), (4, 1, y_done, 6),
        (4, 1, x_done, 10), (4, 3, y_done, 7), (4, 3, x_done, 11), (5, 0, ready, 5), (5, 0, y_done, 8), (5, 1, y_done, 9), (5, 2, y_done, 10), (5, 3, y_done, 11),
    ):
        at(cc, tt, do, p)

    rows = pl.ds(pl.multiple_of(t * block, block), block)

    @pl.when(c < chunks)
    def _():
        for i in range(block // sub):
            at_i = pl.ds(pl.multiple_of(t * block + i * sub, sub), sub)
            a = a_s[at_i]
            for j in range(chunk // 128):
                gate, up = pl.ds(j * 128, 128), pl.ds(chunk + j * 128, 128)
                both = dot(a, jnp.concatenate([gu_s[c, :, gate], gu_s[c, :, up]], 1), 1, 0)
                g, u = both[:, :128], both[:, 128:]
                hid_s[at_i, pl.ds(pl.multiple_of(c * chunk + j * 128, 128), 128)] = (g * sigmoid(g) * u).astype(BF16)

    @pl.when(c == chunks)
    def _():
        added = dot(hid_s[rows], d_s[...], 1, 0).astype(BF16)
        h_ref[...] = (x_ref[...].astype(F32) + added.astype(F32)).astype(BF16)

    at(chunks, steps - 1, ready, *range(chunks + 1, pieces))

    @pl.when((c == chunks) & (t == steps - 1))
    def _():
        for p in range(chunks + 1):
            out_copy(p).wait()


def forward(x, wg, wu, wd, chunk, block, sub):
    (tokens, d), ff = x.shape, wg.shape[-1]
    chunks = ff // chunk
    pieces = 2 * chunks + 2
    sizes = (tokens, d, ff, chunk, chunks, block, sub)
    whole = lambda a: pl.BlockSpec(a.shape, lambda c, t: (0,) * a.ndim, pipeline_mode=pl.Buffered(1))
    dma = pltpu.SemaphoreType.DMA
    return pl.pallas_call(
        functools.partial(forward_kernel, sizes),
        grid=(chunks + 1, tokens // block),
        in_specs=[pl.BlockSpec((block, d), lambda c, t: (jnp.where((c == 0) | (c == chunks), t, 0), 0)), whole(wg), whole(wu), whole(wd)],
        out_specs=[
            pl.BlockSpec((block, d), lambda c, t: (jnp.where(c == chunks, t, 0), 0)),
            pl.BlockSpec(memory_space=pl.ANY),
            pl.BlockSpec(memory_space=pl.ANY),
        ],
        out_shape=[
            jax.ShapeDtypeStruct((tokens, d), BF16),
            jax.ShapeDtypeStruct((2 * chunks, d, 2 * chunk), BF16),
            jax.ShapeDtypeStruct((2, ff, d), BF16),
        ],
        scratch_shapes=[
            pltpu.VMEM((tokens, d), BF16),
            pltpu.VMEM((tokens, ff), BF16),
            pltpu.VMEM((chunks, d, 2 * chunk), BF16),
            pltpu.VMEM((ff, d), BF16),
            dma((pieces, 2)),
            dma((chunks + 1,)),
            dma((pieces, 2)),
            dma((pieces, 2)),
            dma((pieces,)),
            dma((pieces,)),
            dma((pieces, 4)),
            dma((pieces, 4)),
        ],
        compiler_params=pltpu.CompilerParams(collective_id=0, has_side_effects=True, vmem_limit_bytes=VMEM_LIMIT),
        name="forward",
    )(x, wg, wu, wd)


def backward_kernel(sizes, h_ref, dy_ref, x_ref, wgu_ref, wd_ref, gg, gu, gd, a_s, dy_s, da_s, acc_s, mine, c_out, c_in, x_in, y_out, y_in, z_out, z_in,
                    c_sem, x_sem, y_sem, z_sem, d_send, d_recv, l_sem, r_sem):
    tokens, d, ff, chunk, chunks, block, sub = sizes
    last, steps = 2 * chunks - 1, tokens // block
    c, t = pl.program_id(0), pl.program_id(1)
    s, r, other, across, by_y, by_z = places()
    x, core = lax.div(s, 2), lax.rem(s, 2)
    n = d // 4
    rows = pl.ds(pl.multiple_of(t * block, block), block)

    def to_core(k):
        return remote(c_out, c_in.at[lax.rem(k, 2)], c_sem.at[0], c_sem.at[1 + lax.rem(k, 2)], s=other)

    def cols(p):
        return pl.ds(p * chunk, chunk)

    def hop(out, into, sem, k, p, **where):
        return remote(out.at[:, cols(p)], into.at[lax.rem(k, 2), :, cols(p)], sem.at[p, 0], sem.at[p, 1 + lax.rem(k, 2)], **where)

    def to_x(k, p):
        return hop(c_out.at[0], x_in, x_sem, k, p, s=across)

    def to_y(k, p):
        return hop(y_out, y_in, y_sem, k, p, r=by_y)

    def to_z(k, p):
        return hop(z_out, z_in, z_sem, k, p, r=by_z)

    def core_done(k):
        to_core(k).wait()
        c_out[0] = (mine[1 - x] + c_in[lax.rem(k, 2), 1 - x].astype(F32)).astype(BF16)
        for p in range(3):
            to_x(k, p).start()
        mine[x] += c_in[lax.rem(k, 2), x].astype(F32)

    def x_done(k, p):
        to_x(k, p).wait()
        y_out[:, cols(p)] = (mine[x, :, cols(p)] + x_in[lax.rem(k, 2), :, cols(p)].astype(F32)).astype(BF16)
        to_y(k, p).start()

    def y_done(k, p):
        to_y(k, p).wait()
        end_final(k - 1, p)
        z_out[:, cols(p)] = (y_out[:, cols(p)].astype(F32) + y_in[lax.rem(k, 2), :, cols(p)].astype(F32)).astype(BF16)
        to_z(k, p).start()

    def z_done(k, p):
        to_z(k, p).wait()
        z_out[:, cols(p)] = (z_out[:, cols(p)].astype(F32) + z_in[lax.rem(k, 2), :, cols(p)].astype(F32)).astype(BF16)
        start_final(k, p)

    def final(k, p):
        layer, of = 1 - lax.div(k, chunks), lax.rem(k, chunks)
        if p < 2:
            to = (gg, gu)[p].at[layer, :, pl.ds(pl.multiple_of(of * chunk, 128), chunk)]
            return True, pltpu.make_async_copy(z_out.at[:, cols(p)], to, l_sem.at[p]), None
        number = 4 * of + s
        owner, place = lax.div(number, chunks), lax.rem(number, chunks)
        to = gd.at[layer, pl.ds(pl.multiple_of(place * n, 16), n)]
        return owner == s, pltpu.make_async_copy(z_out.at[:, cols(p)], to, l_sem.at[p]), remote(z_out.at[:, cols(p)], to, d_send, d_recv.at[layer, place], s=owner)

    def start_final(k, p):
        stays, local, away = final(k, p)
        if away is None:
            local.start()
        else:
            pl.when(stays)(local.start)
            pl.when(jnp.logical_not(stays))(away.start)

    def end_final(k, p):
        stays, local, away = final(jnp.maximum(k, 0), p)
        pl.when((k >= 0) & stays)(local.wait)
        if away is not None:
            pl.when((k >= 0) & jnp.logical_not(stays))(away.wait_send)

    @pl.when((c == 0) & (t == 0))
    def _():
        load = pltpu.make_async_copy(dy_ref, dy_s, l_sem.at[0])
        load.start()
        greet({"s": other}, {"s": across}, {"s": 3 - s}, {"r": by_y}, {"r": by_z})
        load.wait()

    @pl.when((t == 1) & (c >= 2))
    def _():
        y_done(c - 2, 0)
        y_done(c - 2, 1)

    @pl.when((t == 1) & (c >= 1))
    def _():
        core_done(c - 1)

    @pl.when((t == 2) & (c >= 2))
    def _():
        y_done(c - 2, 2)

    @pl.when((t == steps - 1) & (c >= 1))
    def _():
        x_done(c - 1, 0)
        x_done(c - 1, 1)

    load_x = pltpu.make_async_copy(x_ref.at[rows], a_s.at[rows], r_sem.at[t])

    @pl.when(c == 0)
    def _():
        wide = h_ref[...].astype(F32)
        a_s[rows] = (wide * scale_of(wide)).astype(BF16)
        da_s[:, rows] = jnp.zeros((d, block), F32)

    @pl.when(c == chunks)
    def _():
        load_x.wait()
        wide = a_s[rows].astype(F32)
        a_s[rows] = (wide * scale_of(wide)).astype(BF16)

    @pl.when(t == 0)
    def _():
        acc_s[...] = jnp.zeros_like(acc_s)

    for i in range(block // sub):
        at = pl.ds(pl.multiple_of(t * block + i * sub, sub), sub)
        a, dy = a_s[at], dy_s[at]
        both = dot(a, wgu_ref[0], 1, 0)
        dh = dot(dy, wd_ref[0], 1, 1).astype(BF16).astype(F32)
        g, u = both[:, :chunk], both[:, chunk:]
        sg = sigmoid(g)
        sl = g * sg
        hid = (sl * u).astype(BF16)
        by_u = (dh * sl).astype(BF16)
        by_g = (dh * u * (sg * (1 + g * (1 - sg)))).astype(BF16)
        by_gu = jnp.concatenate([by_g, by_u], 1)
        acc_s[:, : 2 * chunk] += dot(a, by_gu, 0, 0)
        acc_s[:, 2 * chunk :] += dot(hid, dy, 0, 0)

        @pl.when(c < chunks)
        def _():
            da_s[:, at] += dot(wgu_ref[0], by_gu, 1, 1)

    @pl.when(c == chunks - 1)
    def _():
        load_x.start()
        da = da_s[:, rows].T.astype(BF16).astype(F32)
        wide = h_ref[...].astype(F32)
        scale = scale_of(wide)
        along = jnp.sum(da * wide, -1, keepdims=True) * (scale * scale * scale) * (1.0 / d)
        dy_s[rows] = (dy_s[rows].astype(F32) + (da * scale - wide * along).astype(BF16).astype(F32)).astype(BF16)

    @pl.when((t == steps - 1) & (c >= 1))
    def _():
        x_done(c - 1, 2)

    @pl.when((t == steps - 1) & (c >= 2))
    def _():
        for p in range(3):
            z_done(c - 2, p)

    @pl.when(t == steps - 1)
    def _():
        for i in range(2):
            mine[i] = acc_s[pl.ds(pl.multiple_of((2 * i + core) * n, 8), n)]
            c_out[i] = acc_s[pl.ds(pl.multiple_of((2 * i + 1 - core) * n, 8), n)].astype(BF16)
        to_core(c).start()

    @pl.when((c == last) & (t == steps - 1))
    def _():
        core_done(last)
        for do, k, p in (
            (y_done, 1, 0), (y_done, 1, 1), (x_done, 0, 0), (y_done, 1, 2), (x_done, 0, 1), (z_done, 1, 0), (z_done, 1, 1), (x_done, 0, 2),
            (y_done, 0, 0), (z_done, 1, 2), (y_done, 0, 1), (y_done, 0, 2), (z_done, 0, 0), (z_done, 0, 1), (z_done, 0, 2),
        ):
            do(last - k, p)
        for p in range(3):
            end_final(last, p)
        for layer in range(2):
            for place in range(chunks):
                number = s * chunks + place
                to = gd.at[layer, pl.ds(place * n, n)]
                from_other = lax.rem(number, 4) != s
                copy = remote(z_out.at[:, pl.ds(2 * chunk, d)], to, d_send, d_recv.at[layer, place], s=other)
                pl.when(from_other)(copy.wait_recv)


def backward(h, dy, x, wgu, wd, chunk, block, sub):
    (tokens, d), ff = x.shape, wd.shape[1]
    chunks = ff // chunk
    n, last = d // 4, 2 * chunks - 1
    sizes = (tokens, d, ff, chunk, chunks, block, sub)
    dma = pltpu.SemaphoreType.DMA
    wide = 2 * chunk + d
    at = lambda *when: pl.BlockSpec((block, d), lambda c, t: (jnp.where(functools.reduce(jnp.logical_or, [c == w for w in when]), t, 0), 0))
    return pl.pallas_call(
        functools.partial(backward_kernel, sizes),
        grid=(last + 1, tokens // block),
        in_specs=[
            at(0, chunks - 1),
            pl.BlockSpec(memory_space=pl.ANY),
            pl.BlockSpec(memory_space=pl.ANY),
            pl.BlockSpec((1, d, 2 * chunk), lambda c, t: (jnp.minimum(c, last), 0, 0)),
            pl.BlockSpec((1, chunk, d), lambda c, t: (lax.div(jnp.minimum(c, last), chunks), lax.rem(jnp.minimum(c, last), chunks), 0)),
        ],
        out_specs=[pl.BlockSpec(memory_space=pl.ANY)] * 3,
        out_shape=[
            jax.ShapeDtypeStruct((2, n, ff), BF16),
            jax.ShapeDtypeStruct((2, n, ff), BF16),
            jax.ShapeDtypeStruct((2, ff // 4, d), BF16),
        ],
        scratch_shapes=[
            pltpu.VMEM((tokens, d), BF16),
            pltpu.VMEM((tokens, d), BF16),
            pltpu.VMEM((d, tokens), F32),
            pltpu.VMEM((d, wide), F32),
            pltpu.VMEM((2, n, wide), F32),
            pltpu.VMEM((2, n, wide), BF16),
            pltpu.VMEM((2, 2, n, wide), BF16),
            pltpu.VMEM((2, n, wide), BF16),
            pltpu.VMEM((n, wide), BF16),
            pltpu.VMEM((2, n, wide), BF16),
            pltpu.VMEM((n, wide), BF16),
            pltpu.VMEM((2, n, wide), BF16),
            dma((3,)),
            dma((3, 3)),
            dma((3, 3)),
            dma((3, 3)),
            dma,
            dma((2, chunks)),
            dma((3,)),
            dma((tokens // block,)),
        ],
        compiler_params=pltpu.CompilerParams(collective_id=1, has_side_effects=True, vmem_limit_bytes=VMEM_LIMIT),
        name="backward",
    )(h, dy, x, wgu, wd)


def adamw(w, m, v, g):
    m = 0.9 * m + 0.1 * g
    v = 0.95 * v + 0.05 * g * g
    step = m * lax.rsqrt(v + 1e-8) + 0.1 * w
    return (w - 0.02 * step).astype(BF16), m, v


def solution(mesh):
    def step(x, dy, *arrays):
        weights, m, v = (arrays[i : i + 3] for i in (0, 3, 6))
        x, dy = x[0], dy[0]
        h, wgu, wd = forward(x, *weights, 640, 1024, 512)
        gradients = backward(h, dy, x, wgu, wd, 640, 1024, 1024)
        new = [adamw(w.astype(F32), m, v, g.astype(F32)) for w, m, v, g in zip(weights, m, v, gradients, strict=True)]
        return tuple(one[which] for which in range(3) for one in new)

    states, cut = P(("rep", "r", "s"), None, None), P(None, "s", None)
    return jax.shard_map(
        step,
        mesh=mesh,
        in_specs=(states, states) + (cut,) * 9,
        out_specs=(P("rep", "s", None),) * 9,
        check_vma=False,
    )
```
